32 devices in a mesh: dp: 16 (over z, y, x), tensor: 2 (over core).
Axes of the slice: x: 2, y: 2, z: 4, core: 2. Of those that a mesh axis runs over, the one named last changes fastest.
Arguments:
- gradient: bfloat16 [16, 128, 8192], P('dp', 'tensor'), may hold values from -110 to 110
- momentum: bfloat16 [16, 128, 8192], P('dp', 'tensor'), may hold values from -6 to 6
- indices: int32 [16, 2, 128, 32], P('dp', 'tensor'), may hold values from 0 to 4095, all different within a row
Outputs:
- new_momentum: bfloat16 [16, 128, 8192], P('dp', 'tensor')
- update: bfloat16 [128, 8192], P('tensor')
The draws below stay inside these ranges and needn't reach their ends.
Inputs may be any that keep to these rules, and one draw needn't show every extreme that they name: The 32 indices of one span of one replica are distinct; index a * 64 + b names row frequency a and column frequency b.
All inputs are finite; a program needn't handle non-finite values.
Results may differ from the reference program's by a relative error of at most 0.0049.
Values may be sent and summed in bfloat16 or wider, within the bound.
A program may use at most 64 MiB of HBM per device.

```python
import jax
import jax.numpy as jnp
from jax import lax

D = 8192
BLOCK = 64
TOPK = 32
ROWS = 128
REPLICAS = 16


def draw_gradient(key, part):
    keys = jax.random.split(key, 3)
    own = jnp.clip(jax.random.normal(keys[0], (REPLICAS, ROWS, D), jnp.float32), -4.0, 4.0)
    position = jnp.arange(ROWS, dtype=jnp.float32) / ROWS
    rough_rows = jax.random.uniform(keys[1], (ROWS,), jnp.float32, 0.5, 2.0)
    rough_cols = jax.random.uniform(keys[2], (D,), jnp.float32, 0.5, 2.0)
    ramp = 10.0 ** (position - 0.5) * rough_rows
    return (own * ramp[None, :, None] * rough_cols[None, None, :]).astype(jnp.bfloat16)


def levels(rng, extent, shards, least, largest):
    gain, own = 1.0, jax.random.fold_in(rng, 6)
    for dim, parts in shards:
        heights = jnp.exp(jax.random.uniform(jax.random.fold_in(own, dim), (parts,), jnp.float32, least / len(shards), largest / len(shards)))
        gain = gain * jnp.repeat(heights, extent[dim] // parts).reshape([-1 if axis == dim else 1 for axis in range(len(extent))])
    return gain


def choose_distinct(key, rows, amount, top, lift):
    sequence = jax.random.permutation(jax.random.fold_in(key, 1), amount)
    pull = sequence
    for power in range(3):
        pull = pull * pull // amount
    pull = pull * lift // amount
    lots = jax.random.randint(jax.random.fold_in(key, 2), (rows, amount), 0, 4096) + pull
    sure = jax.random.permutation(jax.random.fold_in(key, 3), rows)[jnp.arange(amount) % rows]
    lots = jnp.where(jnp.arange(rows)[:, None] == sure[None, :], 1 << 14, lots)
    priority = lots * amount + jnp.arange(amount)
    return lax.top_k(priority.astype(jnp.int32), top)[1].astype(jnp.int32)


def noise(rng, extent, width, limit, shards=(), kind=jnp.bfloat16):
    loudness = levels(rng, extent, shards, -0.22, 0.18) if shards else 1.0
    array = jax.random.normal(rng, extent, jnp.float32) * width * loudness
    return jnp.minimum(jnp.maximum(array, -limit), limit).astype(kind)


def setup_inputs(seed: int = 0) -> dict:
    arg_keys = jax.random.split(jax.random.key(seed), 4)
    gradient = draw_gradient(jax.random.fold_in(arg_keys[3], 71), 0)
    momentum = noise(arg_keys[1], (REPLICAS, ROWS, D), 1.0, 6.0, ((0, 16), (1, 2)))
    indices = choose_distinct(arg_keys[2], REPLICAS * (ROWS // BLOCK) * (D // BLOCK), BLOCK * BLOCK, TOPK, 0).reshape((REPLICAS, ROWS // BLOCK, D // BLOCK, TOPK))
    return dict(gradient=gradient, momentum=momentum, indices=indices)


EPSILON = 1e-06
DECAY = 0.999

def dct_basis(block_edge):
    frequency = jnp.arange(block_edge, dtype=jnp.float32)[:, None]
    position = jnp.arange(block_edge, dtype=jnp.float32)[None, :]
    waves = jnp.cos(jnp.pi * (2.0 * position + 1.0) * frequency / (2.0 * block_edge))
    weights = jnp.where(frequency == 0.0, jnp.sqrt(1.0 / block_edge), jnp.sqrt(2.0 / block_edge))
    return waves * weights

def reference(gradient, momentum, indices):
    cosines = dct_basis(BLOCK)
    row_blocks = ROWS // BLOCK
    col_blocks = D // BLOCK
    precise = lax.Precision.HIGHEST
    block_rows = jnp.arange(row_blocks, dtype=jnp.int32)[:, None, None]
    block_cols = jnp.arange(col_blocks, dtype=jnp.int32)[None, :, None]

    def to_spans(slab):
        return slab.reshape(row_blocks, BLOCK, col_blocks, BLOCK).transpose(0, 2, 1, 3)

    def from_spans(blocks):
        return blocks.transpose(0, 2, 1, 3).reshape(ROWS, D)

    def compress(operands):
        grad_slab, moment_slab, chosen = operands
        renewed = DECAY * moment_slab.astype(jnp.float32) + grad_slab.astype(jnp.float32)
        spectrum = jnp.einsum('ka,pqab,lb->pqkl', cosines, to_spans(renewed), cosines, precision=precise)
        flattened = spectrum.reshape(row_blocks, col_blocks, BLOCK * BLOCK)
        picked = jnp.take_along_axis(flattened, chosen, axis=2)
        marker = jnp.zeros_like(flattened).at[block_rows, block_cols, chosen].set(1.0)
        retained = (flattened * marker).reshape(row_blocks, col_blocks, BLOCK, BLOCK)
        restored = jnp.einsum('ka,pqkl,lb->pqab', cosines, retained, cosines, precision=precise)
        return ((renewed - from_spans(restored)).astype(jnp.bfloat16), picked.astype(jnp.bfloat16))
    new_momentum, values = lax.map(compress, (gradient, momentum, indices))

    def absorb(running, operands):
        shipped, chosen = operands
        return (running.at[block_rows, block_cols, chosen].add(shipped.astype(jnp.float32)), None)
    start_sum = jnp.zeros((row_blocks, col_blocks, BLOCK * BLOCK), jnp.float32)
    combined, unused = lax.scan(absorb, start_sum, (values, indices))
    combined = combined.reshape(row_blocks, col_blocks, BLOCK, BLOCK)
    decoded = from_spans(jnp.einsum('ka,pqkl,lb->pqab', cosines, combined, cosines, precision=precise))
    spread = jnp.sqrt(jnp.mean(decoded * decoded) + EPSILON)
    update = (decoded / spread).astype(jnp.bfloat16)
    return (new_momentum, update)
```

```python
import functools

import jax
import jax.numpy as jnp
import numpy as np
from jax import lax
from jax.experimental import pallas as pl
from jax.experimental.pallas import tpu as pltpu
from jax.sharding import PartitionSpec as P

BLOCK = 64
LANES = 128
EPSILON = 1e-06
DECAY = 0.999
F32 = jnp.float32
BF16 = jnp.bfloat16
MESH = pl.DeviceIdType.MESH


def dct_basis(edge):
    frequency = np.arange(edge, dtype=np.float64)[:, None]
    position = np.arange(edge, dtype=np.float64)[None, :]
    waves = np.cos(np.pi * (2.0 * position + 1.0) * frequency / (2.0 * edge))
    weights = np.where(frequency == 0.0, np.sqrt(1.0 / edge), np.sqrt(2.0 / edge))
    return (waves * weights).astype(np.float32)


def halves(x):
    high = x.astype(BF16)
    return high, (x - high.astype(F32)).astype(BF16)


def np_halves(x):
    high = x.astype(jnp.bfloat16)
    return high, (x - high.astype(np.float32)).astype(jnp.bfloat16)


def dot(a, b):
    return jnp.dot(a, b, preferred_element_type=F32)


def dot_nt(a, b):
    return lax.dot_general(a, b, (((1,), (1,)), ((), ())), preferred_element_type=F32)


def wide(x, w_high, w_low):
    rows = x.shape[0]
    high, low = halves(x)
    both = dot(jnp.concatenate([high, low], axis=0), w_high)
    return both[:rows] + both[rows:] + dot(high, w_low)


def kernel(
    replicas, shards, unroll, total,
    grad_ref, mom_ref, idx_ref, fwd_ref, inv_ref, rows_ref, rows3_ref,
    newm_ref, upd_ref,
    payload, landed, span_a, span_b, span_v, picks, values, dense, e_out, e_in,
    send_sem, recv_sem, e_send, e_recv,
):
    me = lax.axis_index("dp")
    part = lax.axis_index("tensor")
    barrier = pltpu.get_barrier_semaphore()

    def greet_dp(k, c):
        pl.semaphore_signal(barrier, inc=1, device_id={"dp": lax.rem(me + k, replicas)}, device_id_type=MESH)
        return c

    def greet_tp(k, c):
        pl.semaphore_signal(barrier, inc=1, device_id={"tensor": lax.rem(part + k, shards)}, device_id_type=MESH)
        return c

    lax.fori_loop(1, replicas, greet_dp, 0)
    lax.fori_loop(1, shards, greet_tp, 0)

    topk = idx_ref.shape[1]
    fold = LANES // topk
    width = fold * BLOCK
    groups = grad_ref.shape[1] // width

    chosen = jnp.concatenate(
        [idx_ref[pl.ds(s, groups, stride=fold), :] for s in range(fold)], axis=1
    )
    payload[1] = (chosen // BLOCK).astype(F32).astype(BF16)
    payload[2] = (chosen % BLOCK).astype(F32).astype(BF16)
    picks[0] = chosen // BLOCK
    picks[1] = chosen % BLOCK + BLOCK * (lax.broadcasted_iota(jnp.int32, chosen.shape, 1) // topk)

    tall = lax.broadcasted_iota(jnp.int32, (width, LANES), 0)
    short = lax.broadcasted_iota(jnp.int32, (BLOCK, LANES), 0)

    def masks(g):
        row_hot = (short == picks[0, pl.ds(g, 1), :]).astype(F32).astype(BF16)
        col_hot = (tall == picks[1, pl.ds(g, 1), :]).astype(F32).astype(BF16)
        return row_hot, col_hot

    def columns(g):
        return pl.ds(pl.multiple_of(g * width, width), width)

    def encode(step, c):
        batch = [step * unroll + u for u in range(unroll)]
        for g in batch:
            cols = columns(g)
            renewed = DECAY * mom_ref[:, cols].astype(F32) + grad_ref[:, cols].astype(F32)
            row_hot, col_hot = masks(g)
            part_spec = wide(renewed, fwd_ref[0], fwd_ref[1])
            high, low = halves(part_spec)
            both = dot(jnp.concatenate([high, low], axis=0), col_hot)
            lines = both[:BLOCK] + both[BLOCK:]
            waves = dot(rows_ref[...], jnp.concatenate([row_hot, row_hot], axis=0))
            value = jnp.sum(lines * waves, axis=0, keepdims=True)
            values[pl.ds(g, 1), :] = value
            high, low = halves(waves * value)
            spread = dot_nt(high, col_hot) + dot_nt(low, col_hot)
            restored = wide(spread, inv_ref[0], inv_ref[1])
            newm_ref[:, cols] = (renewed - restored).astype(BF16)
        return c

    lax.fori_loop(0, groups // unroll, encode, 0)
    payload[0] = values[...].astype(BF16)
    pl.semaphore_wait(barrier, replicas - 1 + shards - 1)

    def copy_dp(k, slot):
        return pltpu.make_async_remote_copy(
            src_ref=payload, dst_ref=landed.at[slot],
            send_sem=send_sem.at[k], recv_sem=recv_sem.at[k],
            device_id={"dp": lax.rem(me + k, replicas)}, device_id_type=MESH,
        )

    def start_dp(k, c):
        copy_dp(k, me).start()
        return c

    lax.fori_loop(1, replicas, start_dp, 0)
    landed[me] = payload[...]

    def finish_dp(k, c):
        copy_dp(k, lax.rem(me - k + replicas, replicas)).wait_recv()
        return c

    lax.fori_loop(1, replicas, finish_dp, 0)

    for plane, target in enumerate((span_v, span_a, span_b)):
        for s in range(fold):
            target[s * groups:(s + 1) * groups, :] = jnp.concatenate(
                [landed[r, plane].astype(F32)[:, s * topk:(s + 1) * topk] for r in range(replicas)], axis=1
            )

    depth = replicas * topk
    level = lax.broadcasted_iota(jnp.int32, (BLOCK, depth), 0).astype(F32).astype(BF16)
    zero = jnp.zeros((), BF16)
    one = jnp.ones((), BF16)

    def densify(step, energy):
        tiles = []
        for s in range(fold):
            lines = pl.ds(pl.multiple_of(s * groups + step * 8, 8), 8)
            tiles.append([ref[lines, :] for ref in (span_a, span_b, span_v)])
        for u in range(8):
            blocks = []
            for s in range(fold):
                a, b, v = (tile[u:u + 1].astype(BF16) for tile in tiles[s])
                row_hot = jnp.where(level == a, v, zero)
                col_hot = jnp.where(level == b, one, zero)
                blocks.append(dot_nt(row_hot, col_hot))
            combined = jnp.concatenate(blocks, axis=1)
            dense[:, columns(step * 8 + u)] = combined
            energy = energy + jnp.sum((combined * combined).reshape(BLOCK // 8, 8, width), axis=0)
        return energy

    energy = lax.fori_loop(0, groups // 8, densify, jnp.zeros((8, width), F32))
    energy = sum(energy[:, n * LANES:(n + 1) * LANES] for n in range(width // LANES))
    e_out[...] = energy
    e_in[part] = energy

    def copy_tp(k, slot):
        return pltpu.make_async_remote_copy(
            src_ref=e_out, dst_ref=e_in.at[slot],
            send_sem=e_send.at[k], recv_sem=e_recv.at[k],
            device_id={"tensor": lax.rem(part + k, shards)}, device_id_type=MESH,
        )

    def start_tp(k, c):
        copy_tp(k, part).start()
        return c

    lax.fori_loop(1, shards, start_tp, 0)

    def decode(step, c):
        for u in range(unroll):
            cols = columns(step * unroll + u)
            high, low = halves(wide(dense[:, cols], inv_ref[0], inv_ref[1]))
            dense[:, cols] = dot(rows3_ref[...], jnp.concatenate([high, high, low], axis=0))
        return c

    lax.fori_loop(0, groups // unroll, decode, 0)

    def finish_tp(k, c):
        copy_tp(k, lax.rem(part - k + shards, shards)).wait()
        return c

    lax.fori_loop(1, shards, finish_tp, 0)
    mean = jnp.sum(e_in[...]) / total
    scale = lax.rsqrt(jnp.full((1, width), mean + EPSILON, F32))

    def finish(g, c):
        cols = columns(g)
        upd_ref[:, cols] = (dense[:, cols] * scale).astype(BF16)
        return c

    lax.fori_loop(0, groups, finish, 0)

    def sent_dp(k, c):
        copy_dp(k, me).wait_send()
        return c

    lax.fori_loop(1, replicas, sent_dp, 0)


def local(gradient, momentum, indices, replicas, shards):
    height, cols = gradient.shape[1:]
    topk = indices.shape[-1]
    fold = LANES // topk
    spans = cols // BLOCK
    groups = spans // fold
    assert height == BLOCK and groups * fold == spans
    basis = dct_basis(BLOCK)
    eye = np.eye(fold, dtype=np.float32)
    fwd = jnp.asarray(np.stack(np_halves(np.kron(eye, basis.T))))
    inv = jnp.asarray(np.stack(np_halves(np.kron(eye, basis))))
    high, low = np_halves(basis.T)
    rows = jnp.asarray(np.concatenate([high, low], axis=1))
    rows3 = jnp.asarray(np.concatenate([high, low, high], axis=1))
    depth = max(replicas * topk, LANES)
    vmem = pl.BlockSpec(memory_space=pltpu.VMEM)
    newm, update = pl.pallas_call(
        functools.partial(kernel, replicas, shards, 4, float(height * cols * shards)),
        out_shape=(
            jax.ShapeDtypeStruct((height, cols), BF16),
            jax.ShapeDtypeStruct((height, cols), BF16),
        ),
        in_specs=[vmem] * 7,
        out_specs=(vmem, vmem),
        scratch_shapes=[
            pltpu.VMEM((3, groups, LANES), BF16),
            pltpu.VMEM((replicas, 3, groups, LANES), BF16),
            pltpu.VMEM((spans, depth), F32),
            pltpu.VMEM((spans, depth), F32),
            pltpu.VMEM((spans, depth), F32),
            pltpu.VMEM((2, groups, LANES), jnp.int32),
            pltpu.VMEM((groups, LANES), F32),
            pltpu.VMEM((height, cols), F32),
            pltpu.VMEM((8, LANES), F32),
            pltpu.VMEM((shards, 8, LANES), F32),
            pltpu.SemaphoreType.DMA((replicas,)),
            pltpu.SemaphoreType.DMA((replicas,)),
            pltpu.SemaphoreType.DMA((shards,)),
            pltpu.SemaphoreType.DMA((shards,)),
        ],
        compiler_params=pltpu.CompilerParams(collective_id=0, has_side_effects=True),
        name="demo_step",
    )(gradient[0], momentum[0], indices.reshape(spans, topk), fwd, inv, rows, rows3)
    return newm[None], update


def solution(mesh):
    in_specs = (P("dp", "tensor", None), P("dp", "tensor", None), P("dp", "tensor", None, None))
    out_specs = (P("dp", "tensor", None), P("tensor", None))
    body = functools.partial(local, replicas=mesh.shape["dp"], shards=mesh.shape["tensor"])
    return jax.shard_map(body, mesh=mesh, in_specs=in_specs, out_specs=out_specs, check_vma=False)
```

```python
import functools

import jax
import jax.numpy as jnp
import numpy as np
from jax import lax
from jax.experimental import pallas as pl
from jax.experimental.pallas import tpu as pltpu
from jax.sharding import PartitionSpec as P

BLOCK = 64
LANES = 128
EPSILON = 1e-06
DECAY = 0.999
F32 = jnp.float32
BF16 = jnp.bfloat16
MESH = pl.DeviceIdType.MESH


def dct_basis(edge):
    frequency = np.arange(edge, dtype=np.float64)[:, None]
    position = np.arange(edge, dtype=np.float64)[None, :]
    waves = np.cos(np.pi * (2.0 * position + 1.0) * frequency / (2.0 * edge))
    weights = np.where(frequency == 0.0, np.sqrt(1.0 / edge), np.sqrt(2.0 / edge))
    return (waves * weights).astype(np.float32)


def halves(x):
    high = x.astype(BF16)
    return high, (x - high.astype(F32)).astype(BF16)


def np_halves(x):
    high = x.astype(jnp.bfloat16)
    return high, (x - high.astype(np.float32)).astype(jnp.bfloat16)


def dot(a, b):
    return jnp.dot(a, b, preferred_element_type=F32)


def dot_nt(a, b):
    return lax.dot_general(a, b, (((1,), (1,)), ((), ())), preferred_element_type=F32)


def wide(x, w_high, w_low):
    rows = x.shape[0]
    high, low = halves(x)
    both = dot(jnp.concatenate([high, low], axis=0), w_high)
    return both[:rows] + both[rows:] + dot(high, w_low)


def kernel(
    replicas, shards, unroll, total,
    grad_ref, mom_ref, idx_ref, fwd_ref, inv_ref, rows_ref, rows3_ref,
    newm_ref, upd_ref,
    by_span, picks, values, factor, ids, all_ids, shipped, all_values,
    span_a, span_b, span_v, dense, e_out, e_in,
    id_sem, value_sem, e_send, e_recv,
):
    me = lax.axis_index("dp")
    part = lax.axis_index("tensor")
    barrier = pltpu.get_barrier_semaphore()

    def greet_dp(k, c):
        pl.semaphore_signal(barrier, inc=1, device_id={"dp": lax.rem(me + k, replicas)}, device_id_type=MESH)
        return c

    def greet_tp(k, c):
        pl.semaphore_signal(barrier, inc=1, device_id={"tensor": lax.rem(part + k, shards)}, device_id_type=MESH)
        return c

    lax.fori_loop(1, replicas, greet_dp, 0)
    lax.fori_loop(1, shards, greet_tp, 0)

    topk, spans = idx_ref.shape
    fold = LANES // topk
    width = fold * BLOCK
    groups = spans // fold

    by_span[...] = idx_ref[...].T
    chosen = jnp.concatenate(
        [by_span[pl.ds(s, groups, stride=fold), :] for s in range(fold)], axis=1
    )
    ids[...] = chosen.astype(jnp.int16)
    picks[0] = (chosen // BLOCK).astype(F32)
    slot = lax.broadcasted_iota(jnp.int32, chosen.shape, 1) // topk
    picks[1] = (chosen % BLOCK + BLOCK * slot).astype(F32)

    zero = jnp.zeros((), BF16)
    one = jnp.ones((), BF16)
    tall = lax.broadcasted_iota(jnp.int32, (width, LANES), 0).astype(F32).astype(BF16)
    short = lax.broadcasted_iota(jnp.int32, (BLOCK, LANES), 0).astype(F32).astype(BF16)

    def hot(levels, plane, g):
        return jnp.where(levels == picks[plane, pl.ds(g, 1), :].astype(BF16), one, zero)

    def columns(g, size):
        return pl.ds(pl.multiple_of(g * size, size), size)

    def renew(g):
        cols = columns(g, width)
        return DECAY * mom_ref[:, cols].astype(F32) + grad_ref[:, cols].astype(F32)

    def encode(step, c):
        batch = [step * unroll + u for u in range(unroll)]
        half_spec = wide(jnp.concatenate([renew(g) for g in batch], axis=0), fwd_ref[0], fwd_ref[1])
        high, low = halves(half_spec)
        found = []
        for u, g in enumerate(batch):
            rows = slice(u * BLOCK, (u + 1) * BLOCK)
            both = dot(jnp.concatenate([high[rows], low[rows]], axis=0), hot(tall, 1, g))
            row_hot = hot(short, 0, g)
            waves = dot(rows_ref[...], jnp.concatenate([row_hot, row_hot], axis=0))
            value = jnp.sum((both[:BLOCK] + both[BLOCK:]) * waves, axis=0, keepdims=True)
            found.append((value, halves(waves * value)))
        for g, (value, pair) in zip(batch, found):
            values[pl.ds(g, 1), :] = value
            factor[:, columns(g, 2 * LANES)] = jnp.concatenate(pair, axis=1)
        return c

    def restore(step, c):
        batch = [step * unroll + u for u in range(unroll)]
        spread = []
        for g in batch:
            col_hot = hot(tall, 1, g)
            spread.append(dot_nt(factor[:, columns(g, 2 * LANES)], jnp.concatenate([col_hot, col_hot], axis=1)))
        restored = wide(jnp.concatenate(spread, axis=0), inv_ref[0], inv_ref[1])
        for u, g in enumerate(batch):
            newm_ref[:, columns(g, width)] = (renew(g) - restored[u * BLOCK:(u + 1) * BLOCK]).astype(BF16)
        return c

    def copy_dp(src, dst, sems, k, slot):
        return pltpu.make_async_remote_copy(
            src_ref=src, dst_ref=dst.at[slot],
            send_sem=sems.at[0, k], recv_sem=sems.at[1, k],
            device_id={"dp": lax.rem(me + k, replicas)}, device_id_type=MESH,
        )

    def to_all(src, dst, sems):
        def start(k, c):
            copy_dp(src, dst, sems, k, me).start()
            return c
        lax.fori_loop(1, replicas, start, 0)
        dst[me] = src[...]

    def from_all(src, dst, sems):
        def finish(k, c):
            copy_dp(src, dst, sems, k, lax.rem(me - k + replicas, replicas)).wait_recv()
            return c
        lax.fori_loop(1, replicas, finish, 0)

    def sent_all(src, dst, sems):
        def finish(k, c):
            copy_dp(src, dst, sems, k, me).wait_send()
            return c
        lax.fori_loop(1, replicas, finish, 0)

    steps = groups // unroll
    lax.fori_loop(0, steps // 2, encode, 0)
    pl.semaphore_wait(barrier, replicas - 1 + shards - 1)
    to_all(ids, all_ids, id_sem)
    lax.fori_loop(steps // 2, steps, encode, 0)
    shipped[...] = values[...].astype(BF16)
    to_all(shipped, all_values, value_sem)
    lax.fori_loop(0, steps, restore, 0)
    from_all(ids, all_ids, id_sem)
    from_all(shipped, all_values, value_sem)

    for s in range(fold):
        lines = slice(s * groups, (s + 1) * groups)
        lanes = slice(s * topk, (s + 1) * topk)
        span_v[lines, :] = jnp.concatenate([all_values[r].astype(F32)[:, lanes] for r in range(replicas)], axis=1)
        named = jnp.concatenate([all_ids[r].astype(jnp.int32)[:, lanes] for r in range(replicas)], axis=1)
        span_a[lines, :] = (named // BLOCK).astype(F32)
        span_b[lines, :] = (named % BLOCK).astype(F32)

    depth = replicas * topk
    level = lax.broadcasted_iota(jnp.int32, (BLOCK, depth), 0).astype(F32).astype(BF16)

    def densify(step, energy):
        tiles = []
        for s in range(fold):
            lines = pl.ds(pl.multiple_of(s * groups + step * 8, 8), 8)
            tiles.append([ref[lines, :] for ref in (span_a, span_b, span_v)])
        for u in range(8):
            blocks = []
            for s in range(fold):
                a, b, v = (tile[u:u + 1].astype(BF16) for tile in tiles[s])
                row_hot = jnp.where(level == a, v, zero)
                col_hot = jnp.where(level == b, one, zero)
                blocks.append(dot_nt(row_hot, col_hot))
            combined = jnp.concatenate(blocks, axis=1)
            dense[:, columns(step * 8 + u, width)] = combined
            energy = energy + jnp.sum((combined * combined).reshape(BLOCK // 8, 8, width), axis=0)
        return energy

    energy = lax.fori_loop(0, groups // 8, densify, jnp.zeros((8, width), F32))
    energy = sum(energy[:, n * LANES:(n + 1) * LANES] for n in range(width // LANES))
    e_out[...] = energy
    e_in[part] = energy

    def copy_tp(k, slot):
        return pltpu.make_async_remote_copy(
            src_ref=e_out, dst_ref=e_in.at[slot],
            send_sem=e_send.at[k], recv_sem=e_recv.at[k],
            device_id={"tensor": lax.rem(part + k, shards)}, device_id_type=MESH,
        )

    def start_tp(k, c):
        copy_tp(k, part).start()
        return c

    lax.fori_loop(1, shards, start_tp, 0)

    def decode(step, c):
        batch = [columns(step * unroll + u, width) for u in range(unroll)]
        across = wide(jnp.concatenate([dense[:, cols] for cols in batch], axis=0), inv_ref[0], inv_ref[1])
        high, low = halves(across)
        done = []
        for u in range(unroll):
            rows = slice(u * BLOCK, (u + 1) * BLOCK)
            done.append(dot(rows3_ref[...], jnp.concatenate([high[rows], high[rows], low[rows]], axis=0)))
        for cols, block in zip(batch, done):
            dense[:, cols] = block
        return c

    lax.fori_loop(0, groups // unroll, decode, 0)

    def finish_tp(k, c):
        copy_tp(k, lax.rem(part - k + shards, shards)).wait()
        return c

    lax.fori_loop(1, shards, finish_tp, 0)
    mean = jnp.sum(e_in[...]) / total
    scale = lax.rsqrt(jnp.full((1, width), mean + EPSILON, F32))

    def finish(step, c):
        for u in range(unroll):
            cols = columns(step * unroll + u, width)
            upd_ref[:, cols] = (dense[:, cols] * scale).astype(BF16)
        return c

    lax.fori_loop(0, groups // unroll, finish, 0)
    sent_all(ids, all_ids, id_sem)
    sent_all(shipped, all_values, value_sem)


def local(gradient, momentum, indices, replicas, shards):
    height, cols = gradient.shape[1:]
    topk = indices.shape[-1]
    fold = LANES // topk
    spans = cols // BLOCK
    groups = spans // fold
    assert height == BLOCK and groups * fold == spans
    basis = dct_basis(BLOCK)
    eye = np.eye(fold, dtype=np.float32)
    fwd = jnp.asarray(np.stack(np_halves(np.kron(eye, basis.T))))
    inv = jnp.asarray(np.stack(np_halves(np.kron(eye, basis))))
    high, low = np_halves(basis.T)
    rows = jnp.asarray(np.concatenate([high, low], axis=1))
    rows3 = jnp.asarray(np.concatenate([high, low, high], axis=1))
    depth = max(replicas * topk, LANES)
    vmem = pl.BlockSpec(memory_space=pltpu.VMEM)
    newm, update = pl.pallas_call(
        functools.partial(kernel, replicas, shards, 8, float(height * cols * shards)),
        out_shape=(
            jax.ShapeDtypeStruct((height, cols), BF16),
            jax.ShapeDtypeStruct((height, cols), BF16),
        ),
        in_specs=[vmem] * 7,
        out_specs=(vmem, vmem),
        scratch_shapes=[
            pltpu.VMEM((spans, topk), jnp.int32),
            pltpu.VMEM((2, groups, LANES), F32),
            pltpu.VMEM((groups, LANES), F32),
            pltpu.VMEM((height, groups * 2 * LANES), BF16),
            pltpu.VMEM((groups, LANES), jnp.int16),
            pltpu.VMEM((replicas, groups, LANES), jnp.int16),
            pltpu.VMEM((groups, LANES), BF16),
            pltpu.VMEM((replicas, groups, LANES), BF16),
            pltpu.VMEM((spans, depth), F32),
            pltpu.VMEM((spans, depth), F32),
            pltpu.VMEM((spans, depth), F32),
            pltpu.VMEM((height, cols), F32),
            pltpu.VMEM((8, LANES), F32),
            pltpu.VMEM((shards, 8, LANES), F32),
            pltpu.SemaphoreType.DMA((2, replicas)),
            pltpu.SemaphoreType.DMA((2, replicas)),
            pltpu.SemaphoreType.DMA((shards,)),
            pltpu.SemaphoreType.DMA((shards,)),
        ],
        compiler_params=pltpu.CompilerParams(collective_id=0, has_side_effects=True),
        name="demo_step",
    )(gradient[0], momentum[0], indices.reshape(spans, topk).T, fwd, inv, rows, rows3)
    return newm[None], update


def solution(mesh):
    in_specs = (P("dp", "tensor", None), P("dp", "tensor", None), P("dp", "tensor", None, None))
    out_specs = (P("dp", "tensor", None), P("tensor", None))
    body = functools.partial(local, replicas=mesh.shape["dp"], shards=mesh.shape["tensor"])
    return jax.shard_map(body, mesh=mesh, in_specs=in_specs, out_specs=out_specs, check_vma=False)
```
